128 devices in a mesh: freq: 4 (over x), shot: 32 (over y, z, core).
Axes of the slice: x: 4, y: 4, z: 4, core: 2. Of those that a mesh axis runs over, the one named last changes fastest.
Arguments:
- traces: bfloat16 [2, 4, 3072, 3072], P(None, 'freq', 'shot'), may hold values from -40 to 40, as said below
Outputs:
- multiples: bfloat16 [2, 4, 3072, 3072], P(None, 'freq', 'shot')
- primaries: bfloat16 [2, 4, 3072, 3072], P(None, 'freq', 'shot')
The draws below stay inside these ranges and needn't reach their ends.
Inputs may be any that keep to these rules, and one draw needn't show every extreme that they name: `traces`: finite recorded data.
All inputs are finite; a program needn't handle non-finite values.
Results may differ from the reference program's by a relative error of at most 0.0005.
Values may be sent and summed in bfloat16 or wider, within the bound.
A program may use at most 192 MiB of HBM per device.

```python
import math
import jax
import jax.numpy as jnp
from jax import lax

NRECV = 3072
FREQS = 4


def draw_traces(key, part):
    row_index = jnp.arange(NRECV, dtype=jnp.float32)
    row_ramp = jnp.sqrt(1.0 + 2.0 * row_index / (NRECV - 1))

    def per_band(freq_index):
        band_key = jax.random.fold_in(key, freq_index + 17)
        noise_key, scale_key = jax.random.split(band_key)
        noise = jnp.clip(jax.random.normal(noise_key, (2, NRECV, NRECV), jnp.float32), -4.0, 4.0)
        row_scale = jnp.exp(jax.random.uniform(scale_key, (NRECV,), jnp.float32, math.log(0.4), math.log(4.0)))
        base = noise * (0.3 * 0.70710678 * row_scale * row_ramp)[None, :, None]
        base_re = base[0]
        base_im = base[1]
        square_re = jnp.dot(base_re, base_re, precision=lax.Precision.HIGHEST) - jnp.dot(base_im, base_im, precision=lax.Precision.HIGHEST)
        square_im = jnp.dot(base_re, base_im, precision=lax.Precision.HIGHEST) + jnp.dot(base_im, base_re, precision=lax.Precision.HIGHEST)
        amplitude = 1.0 + 0.35 * freq_index.astype(jnp.float32) / (FREQS - 1)
        factor = 0.5 / math.sqrt(NRECV)
        return amplitude * jnp.stack([base_re + factor * square_re, base_im + factor * square_im])
    stacked = lax.map(per_band, jnp.arange(FREQS))
    return jnp.clip(jnp.transpose(stacked, (1, 0, 2, 3)), -40.0, 40.0).astype(jnp.bfloat16)


def setup_inputs(seed: int = 0) -> dict:
    seeds = jax.random.split(jax.random.key(seed), 2)
    traces = draw_traces(jax.random.fold_in(seeds[1], 71), 0)
    return dict(traces=traces)


epsilon = 1e-06

def reference(traces):
    factor = 1.0 / math.sqrt(NRECV)
    data = traces.astype(jnp.float32)

    def per_band(freq_index):
        data_re = data[0, freq_index]
        data_im = data[1, freq_index]
        mult_re = (jnp.dot(data_re, data_re, precision=lax.Precision.HIGHEST) - jnp.dot(data_im, data_im, precision=lax.Precision.HIGHEST)) * factor
        mult_im = (jnp.dot(data_re, data_im, precision=lax.Precision.HIGHEST) + jnp.dot(data_im, data_re, precision=lax.Precision.HIGHEST)) * factor
        return jnp.stack([mult_re, mult_im])
    mult = lax.map(per_band, jnp.arange(FREQS))
    mult = jnp.transpose(mult, (1, 0, 2, 3))
    mult_re = mult[0]
    mult_im = mult[1]
    data_re = data[0]
    data_im = data[1]
    total_count = float(FREQS * NRECV * NRECV)
    num_re = jnp.sum(mult_re * data_re + mult_im * data_im) / total_count
    num_im = jnp.sum(mult_re * data_im - mult_im * data_re) / total_count
    denom = jnp.sum(mult_re * mult_re + mult_im * mult_im) / total_count + epsilon
    fit_re = num_re / denom
    fit_im = num_im / denom
    prim_re = data_re - (fit_re * mult_re - fit_im * mult_im)
    prim_im = data_im - (fit_re * mult_im + fit_im * mult_re)
    primaries = jnp.stack([prim_re, prim_im]).astype(jnp.bfloat16)
    return (mult.astype(jnp.bfloat16), primaries)
```

```python
import functools
import math

import jax
import jax.numpy as jnp
from jax import lax
from jax.experimental import pallas as pl
from jax.experimental.pallas import tpu as pltpu
from jax.sharding import PartitionSpec as P

epsilon = 1e-06
SIDE = 4
MESH = pl.DeviceIdType.MESH


def kernel(
    dims, x_ref, mult_ref, prim_ref,
    a, b, stage, prod, own, ostage, om, op, fita, fitb,
    local_sems,
    a_send, a_recv, b_send, b_recv, d_send, d_recv, o_send, o_recv,
    fa_send, fa_recv, fb_send, fb_recv,
):
    freqs, rows, order, width, chunks = dims
    block = order // SIDE
    scale = 1.0 / math.sqrt(order)
    f = lax.axis_index("freq")
    s = lax.axis_index("shot")
    c = lax.rem(s, 2)
    z = lax.rem(s // 2, SIDE)
    y = s // (2 * SIDE)
    p = z * (1 - c) + y * c
    q = y * (1 - c) + z * c

    def dev(qq, pp):
        return (1 - c) * ((qq * SIDE + pp) * 2) + c * ((pp * SIDE + qq) * 2 + 1)

    def turn(i, d):
        return lax.rem(i + d + SIDE, SIDE)

    sib = s + 1 - 2 * c
    pr, pl_, pfar = turn(p, 1), turn(p, -1), turn(p, 2)
    qr, ql, qfar = turn(q, 1), turn(q, -1), turn(q, 2)

    def cols(qq, pp, j):
        return pl.ds(pl.multiple_of(lax.rem(qq + pp, SIDE) * block + j * width, 128), width)

    def remote(src, dst, ss, rs, shot):
        return pltpu.make_async_remote_copy(
            src_ref=src, dst_ref=dst, send_sem=ss, recv_sem=rs,
            device_id={"shot": shot}, device_id_type=MESH,
        )

    load = pltpu.make_async_copy(x_ref, a.at[:, p], local_sems.at[0])
    load.start()

    barrier = pltpu.get_barrier_semaphore()
    partners = 0
    for i in range(SIDE):
        for k in range(SIDE):
            if i or k:
                pl.semaphore_signal(
                    barrier, inc=1, device_id={"shot": dev(turn(q, i), turn(p, k))}, device_id_type=MESH
                )
                partners += 1
    for i in range(freqs):
        for other in (0, 1):
            if i or other:
                pl.semaphore_signal(
                    barrier, inc=1,
                    device_id={"freq": lax.rem(f + i, freqs), "shot": sib if other else s},
                    device_id_type=MESH,
                )
                partners += 1
    pl.semaphore_wait(barrier, partners)
    load.wait()

    sent = []

    def go(copy):
        copy.start()
        sent.append(copy)
        return copy

    right, left = dev(q, pr), dev(q, pl_)
    ar = [go(remote(a.at[h, p], a.at[h, p], a_send.at[h], a_recv.at[h], right)) for h in (0, 1)]
    al = {h: go(remote(a.at[h, p], a.at[h, p], a_send.at[2 + h], a_recv.at[2 + h], left)) for h in (1, 0)}

    def from_left(h):
        return remote(a.at[h, pl_], a.at[h, pl_], a_send.at[h], a_recv.at[h], right)

    def from_right(h):
        return remote(a.at[h, pr], a.at[h, pr], a_send.at[2 + h], a_recv.at[2 + h], left)

    def far(h):
        return remote(a.at[h, pfar], a.at[h, pfar], a_send.at[4 + h], a_recv.at[4 + h], right)

    qright, qleft = dev(qr, p), dev(ql, p)
    ring = [p, pr, pl_, pfar]

    def b_own(j, r):
        pp = ring[r]
        return pltpu.make_async_copy(
            a.at[:, pp, :, cols(q, p, j)], b.at[j, :, dev(q, pp)], local_sems.at[1 + j * SIDE + r]
        )

    def b_dir(j, r, d):
        pp = ring[r]
        return remote(
            a.at[:, pp, :, cols(qr if d == 0 else ql, p, j)], b.at[j, :, dev(q, pp)],
            b_send.at[j, r, d], b_recv.at[j, r, d], qright if d == 0 else qleft,
        )

    def b_stage(j, r, h):
        pp = ring[r]
        return remote(
            a.at[h, pp, :, cols(qfar, p, j)], stage.at[j, h, r],
            b_send.at[j, r, 2 + h], b_recv.at[j, r, 2 + h], qright if h == 0 else qleft,
        )

    def b_fwd(j, r, h):
        pp = ring[r]
        return remote(
            stage.at[j, h, r], b.at[j, h, dev(ql if h == 0 else qr, pp)],
            b_send.at[j, r, 4 + h], b_recv.at[j, r, 4 + h], qright if h == 0 else qleft,
        )

    def d2d(j, r, k):
        kb = dev([q, qr, ql, qfar][k], ring[r])
        return remote(b.at[j, :, kb], b.at[j, :, kb], d_send.at[j, r, k], d_recv.at[j, r, k], sib)

    def d2d_src(j, r, k):
        sq, sp = p, q
        kk = turn(sq, [0, 1, -1, 2][k])
        rr = turn(sp, [0, 1, -1, 2][r])
        kb = c * ((kk * SIDE + rr) * 2) + (1 - c) * ((rr * SIDE + kk) * 2 + 1)
        return remote(b.at[j, :, kb], b.at[j, :, kb], d_send.at[j, r, k], d_recv.at[j, r, k], sib)

    locals_ = []

    def send_b(j, r):
        for h in (0, 1):
            go(b_stage(j, r, h))
        for d in (0, 1):
            go(b_dir(j, r, d))
        copy = b_own(j, r)
        copy.start()
        locals_.append(copy)

    def forward_b(j, r):
        for h in (0, 1):
            b_stage(j, r, h).wait_recv()
            go(b_fwd(j, r, h))

    send_b(0, 0)
    from_left(0).wait_recv()
    go(remote(a.at[0, pl_], a.at[0, pl_], a_send.at[4], a_recv.at[4], right))
    from_right(1).wait_recv()
    go(remote(a.at[1, pr], a.at[1, pr], a_send.at[5], a_recv.at[5], left))
    forward_b(0, 0)
    from_left(1).wait_recv()
    from_right(0).wait_recv()
    send_b(0, 1)
    send_b(0, 2)
    far(0).wait_recv()
    far(1).wait_recv()
    send_b(0, 3)
    for j in range(1, chunks):
        for r in range(SIDE):
            send_b(j, r)
    for r in range(1, SIDE):
        forward_b(0, r)

    def o_dir(j, d):
        return remote(
            prod.at[j, :, pr if d == 0 else pl_], own.at[:, :, cols(q, p, j)],
            o_send.at[j, d], o_recv.at[j, d], right if d == 0 else left,
        )

    def o_stage(j, h):
        return remote(
            prod.at[j, h, pfar], ostage.at[j, h],
            o_send.at[j, 2 + h], o_recv.at[j, 2 + h], right if h == 0 else left,
        )

    def o_fwd(j, h):
        return remote(
            ostage.at[j, h], own.at[h, :, cols(q, pl_ if h == 0 else pr, j)],
            o_send.at[j, 4 + h], o_recv.at[j, 4 + h], right if h == 0 else left,
        )

    def o_own(j):
        return pltpu.make_async_copy(
            prod.at[j, :, p], own.at[:, :, cols(q, p, j)], local_sems.at[1 + chunks * SIDE + j]
        )

    def forward_o(j):
        for h in (0, 1):
            o_stage(j, h).wait_recv()
            go(o_fwd(j, h))

    sums = [jnp.zeros((8, width), jnp.float32) for _ in range(3)]
    depth = SIDE * SIDE * 2 * rows
    for j in range(chunks):
        for r in range(SIDE):
            locals_[j * SIDE + r].wait()
            go(d2d(j, r, 0))
        for r in range(SIDE):
            for d in (0, 1):
                b_dir(j, r, d).wait_recv()
                go(d2d(j, r, 2 if d == 0 else 1))
        for r in range(SIDE):
            for h in (0, 1):
                b_fwd(j, r, h).wait_recv()
            go(d2d(j, r, 3))
        if j + 1 < chunks:
            for r in range(SIDE):
                forward_b(j + 1, r)
        for r in range(SIDE):
            for k in range(SIDE):
                d2d_src(j, r, k).wait_recv()
        here = cols(q, p, j)
        br = b[j, 0].reshape(depth, width)
        bi = b[j, 1].reshape(depth, width)
        for half in range(2):
            at = pl.ds(half * 2, 2)
            lhs = a[:, at].reshape(4 * rows, depth)
            xr = jnp.dot(lhs, br, preferred_element_type=jnp.float32)
            xi = jnp.dot(lhs, bi, preferred_element_type=jnp.float32)
            mr = (xr[: 2 * rows] - xi[2 * rows :]) * scale
            mi = (xi[: 2 * rows] + xr[2 * rows :]) * scale
            prod[j, 0, at] = mr.reshape(2, rows, width)
            prod[j, 1, at] = mi.reshape(2, rows, width)
            dr = a[0, at, :, here].reshape(2 * rows, width).astype(jnp.float32)
            di = a[1, at, :, here].reshape(2 * rows, width).astype(jnp.float32)
            terms = (mr * dr + mi * di, mr * di - mi * dr, mr * mr + mi * mi)
            sums = [u + jnp.sum(t.reshape(-1, 8, width), axis=0) for u, t in zip(sums, terms)]
        for h in (0, 1):
            go(o_stage(j, h))
        for d in (0, 1):
            go(o_dir(j, d))
        copy = o_own(j)
        copy.start()
        locals_.append(copy)
        if j:
            forward_o(j - 1)

    line = [jnp.sum(u.reshape(8, width // 128, 128).sum(axis=1), axis=0, keepdims=True) for u in sums]
    me = q * SIDE + p
    fita[me] = jnp.concatenate(line + [jnp.zeros((5, 128), jnp.float32)], axis=0)

    def fa(i, k, back=False):
        to = dev(turn(q, i), turn(p, k))
        slot = me if not back else turn(q, -i) * SIDE + turn(p, -k)
        n = i * SIDE + k
        return remote(fita.at[slot], fita.at[slot], fa_send.at[n], fa_recv.at[n], to)

    pairs = [(i, k) for i in range(SIDE) for k in range(SIDE) if i or k]
    for i, k in pairs:
        go(fa(i, k))
    forward_o(chunks - 1)
    for i, k in pairs:
        fa(i, k, True).wait_recv()
    group = jnp.sum(fita[...], axis=0)
    mine = f * 2 + c
    fitb[mine] = group

    def fb(i, other, back=False):
        cc = c if not other else 1 - c
        slot = mine if not back else lax.rem(f - i + freqs, freqs) * 2 + cc
        n = i * 2 + other
        return pltpu.make_async_remote_copy(
            src_ref=fitb.at[slot], dst_ref=fitb.at[slot], send_sem=fb_send.at[n], recv_sem=fb_recv.at[n],
            device_id={"freq": lax.rem(f + i, freqs), "shot": sib if other else s}, device_id_type=MESH,
        )

    others = [(i, o) for i in range(freqs) for o in (0, 1) if i or o]
    for i, o in others:
        go(fb(i, o))

    for j in range(chunks):
        locals_[chunks * SIDE + j].wait()
        for d in (0, 1):
            o_dir(j, d).wait_recv()
        for h in (0, 1):
            o_fwd(j, h).wait_recv()
    om[...] = own[...].astype(jnp.bfloat16)
    out_m = pltpu.make_async_copy(om, mult_ref, local_sems.at[0])
    out_m.start()

    for i, o in others:
        fb(i, o, True).wait_recv()
    total = jnp.sum(fitb[...], axis=0)
    total = jnp.sum(total, axis=1, keepdims=True)
    count = float(freqs * order * order)
    den = total[2:3] / count + epsilon
    fit_re = total[0:1] / count / den
    fit_im = total[1:2] / count / den
    for t in range(0, order, 512):
        at = pl.ds(t, 512)
        mr, mi = own[0, :, at], own[1, :, at]
        op[0, :, at] = (a[0, p, :, at].astype(jnp.float32) - (fit_re * mr - fit_im * mi)).astype(jnp.bfloat16)
        op[1, :, at] = (a[1, p, :, at].astype(jnp.float32) - (fit_re * mi + fit_im * mr)).astype(jnp.bfloat16)
    out_p = pltpu.make_async_copy(op, prim_ref, local_sems.at[1])
    out_p.start()
    for copy in sent:
        copy.wait_send()
    out_m.wait()
    out_p.wait()


def per_device(traces):
    rows, order = traces.shape[2], traces.shape[3]
    freqs = lax.axis_size("freq")
    block = order // SIDE
    width = 256 if block % 256 == 0 else 128
    chunks = block // width
    dma = pltpu.SemaphoreType.DMA
    out = jax.ShapeDtypeStruct((2, rows, order), jnp.bfloat16)
    shots = SIDE * SIDE * 2
    mult, prim = pl.pallas_call(
        functools.partial(kernel, (freqs, rows, order, width, chunks)),
        out_shape=(out, out),
        in_specs=[pl.BlockSpec(memory_space=pl.ANY)],
        out_specs=(pl.BlockSpec(memory_space=pl.ANY), pl.BlockSpec(memory_space=pl.ANY)),
        scratch_shapes=[
            pltpu.VMEM((2, SIDE, rows, order), jnp.bfloat16),
            pltpu.VMEM((chunks, 2, shots, rows, width), jnp.bfloat16),
            pltpu.VMEM((chunks, 2, SIDE, rows, width), jnp.bfloat16),
            pltpu.VMEM((chunks, 2, SIDE, rows, width), jnp.float32),
            pltpu.VMEM((2, rows, order), jnp.float32),
            pltpu.VMEM((chunks, 2, rows, width), jnp.float32),
            pltpu.VMEM((2, rows, order), jnp.bfloat16),
            pltpu.VMEM((2, rows, order), jnp.bfloat16),
            pltpu.VMEM((SIDE * SIDE, 8, 128), jnp.float32),
            pltpu.VMEM((freqs * 2, 8, 128), jnp.float32),
            dma((1 + chunks * SIDE + chunks,)),
            dma((6,)), dma((6,)),
            dma((chunks, SIDE, 6)), dma((chunks, SIDE, 6)),
            dma((chunks, SIDE, SIDE)), dma((chunks, SIDE, SIDE)),
            dma((chunks, 6)), dma((chunks, 6)),
            dma((SIDE * SIDE,)), dma((SIDE * SIDE,)),
            dma((freqs * 2,)), dma((freqs * 2,)),
        ],
        compiler_params=pltpu.CompilerParams(
            collective_id=0, has_side_effects=True, vmem_limit_bytes=60 * 1024 * 1024
        ),
    )(traces.reshape(2, rows, order))
    return mult.reshape(traces.shape), prim.reshape(traces.shape)


def solution(mesh):
    placed = P(None, "freq", "shot", None)
    return jax.shard_map(
        per_device,
        mesh=mesh,
        in_specs=(placed,),
        out_specs=(placed, placed),
        check_vma=False,
    )
```

```python
import functools
import math

import jax
import jax.numpy as jnp
from jax import lax
from jax.experimental import pallas as pl
from jax.experimental.pallas import tpu as pltpu
from jax.sharding import PartitionSpec as P

epsilon = 1e-06
SIDE = 4
MESH = pl.DeviceIdType.MESH
STEPS = (0, 1, -1, 2)


def kernel(dims, x_ref, mult_ref, prim_ref, *refs):
    freqs, rows, order, widths = dims
    chunks = len(widths)
    starts = [sum(widths[:j]) for j in range(chunks)]
    a, own, fit = refs[:3]
    b = refs[3 : 3 + chunks]
    prod = refs[3 + chunks : 3 + 2 * chunks]
    load_sem, own_sem, a_send, a_recv, b_send, b_recv, d_send, d_recv, o_send, o_recv, f_send, f_recv = refs[
        3 + 2 * chunks :
    ]
    block = order // SIDE
    scale = 1.0 / math.sqrt(order)
    f = lax.axis_index("freq")
    s = lax.axis_index("shot")
    c = lax.rem(s, 2)
    z = lax.rem(s // 2, SIDE)
    y = s // (2 * SIDE)
    p = z * (1 - c) + y * c
    q = y * (1 - c) + z * c

    def dev(qq, pp):
        return (1 - c) * ((qq * SIDE + pp) * 2) + c * ((pp * SIDE + qq) * 2 + 1)

    def turn(i, d):
        return lax.rem(i + d + SIDE, SIDE)

    sib = s + 1 - 2 * c
    ps = [turn(p, d) for d in STEPS]
    qs = [turn(q, d) for d in STEPS]
    pdev = [{"shot": dev(q, pp)} for pp in ps]
    qdev = [{"shot": dev(qq, p)} for qq in qs]
    xdev = [{"freq": lax.rem(f + i, freqs)} for i in range(freqs)]
    back = (0, 2, 1, 3)

    def cols(qq, pp, j):
        return pl.ds(pl.multiple_of(lax.rem(qq + pp, SIDE) * block + starts[j], 128), widths[j])

    def remote(src, dst, ss, rs, to):
        return pltpu.make_async_remote_copy(
            src_ref=src, dst_ref=dst, send_sem=ss, recv_sem=rs, device_id=to, device_id_type=MESH
        )

    load = pltpu.make_async_copy(x_ref, a.at[:, p], load_sem)
    load.start()

    barrier = pltpu.get_barrier_semaphore()
    near = pdev[1:] + qdev[1:] + [{"shot": sib}] + xdev[1:]
    for to in near:
        pl.semaphore_signal(barrier, inc=1, device_id=to, device_id_type=MESH)
    pl.semaphore_wait(barrier, len(near))
    load.wait()

    sent = []

    def go(copy):
        copy.start()
        sent.append(copy)
        return copy

    def a_copy(n, backward=False):
        h = (0, 1, 1, 0, 0, 1)[n]
        k = (0, 0, 0, 0, 2, 1)[n]
        to = (1, 1, 2, 2, 1, 2)[n]
        if backward:
            k = (2, 2, 1, 1, 3, 3)[n]
        here = a.at[h, ps[k]]
        return remote(here, here, a_send.at[n], a_recv.at[n], pdev[to])

    def b_own(j, r):
        return pltpu.make_async_copy(
            a.at[:, ps[r], :, cols(q, p, j)], b[j].at[:, dev(q, ps[r])], own_sem.at[j, r]
        )

    def b_copy(j, r, k):
        return remote(
            a.at[:, ps[r], :, cols(qs[k], p, j)], b[j].at[:, dev(q, ps[r])],
            b_send.at[j, r, k], b_recv.at[j, r, k], qdev[k],
        )

    def d_copy(j, r, k):
        kb = dev(qs[k], ps[r])
        here = b[j].at[:, kb]
        return remote(here, here, d_send.at[j, r, k], d_recv.at[j, r, k], {"shot": sib})

    def send_b(j, r):
        for k in (3, 1, 2):
            go(b_copy(j, r, k))
        b_own(j, r).start()

    for n in (0, 2, 1, 3):
        go(a_copy(n))
    send_b(0, 0)
    for n in (0, 2):
        a_copy(n, True).wait_recv()
        go(a_copy(n // 2 + 4))
    for n in (1, 3):
        a_copy(n, True).wait_recv()
    send_b(0, 1)
    send_b(0, 2)
    for n in (4, 5):
        a_copy(n, True).wait_recv()
    send_b(0, 3)
    for j in range(1, chunks):
        for r in range(SIDE):
            send_b(j, r)

    def o_copy(j, k):
        return remote(
            prod[j].at[:, ps[k]], own.at[:, :, cols(q, p, j)], o_send.at[j, k], o_recv.at[j, k], pdev[k]
        )

    def send_o(j):
        for k in (3, 1, 2):
            go(o_copy(j, k))

    sums = [jnp.zeros((8, 128), jnp.float32) for _ in range(3)]
    depth = SIDE * SIDE * 2 * rows
    for j in range(chunks):
        width = widths[j]
        for r in range(SIDE):
            b_own(j, r).wait()
            go(d_copy(j, r, 0))
        for r in range(SIDE):
            for k in (3, 1, 2):
                b_copy(j, r, k).wait_recv()
                go(d_copy(j, r, back[k]))
        if j == chunks - 1:
            for i in range(j):
                send_o(i)
        for r in range(SIDE):
            for k in range(SIDE):
                d_copy(j, r, k).wait_recv()
        here = cols(q, p, j)
        br = b[j][0].reshape(depth, width)
        bi = b[j][1].reshape(depth, width)
        for half in range(2):
            at = pl.ds(half * 2, 2)
            lhs = a[:, at].reshape(4 * rows, depth)
            if width == 128:
                x = jnp.dot(lhs, jnp.concatenate([br, bi], axis=1), preferred_element_type=jnp.float32)
                xr, xi = x[:, :128], x[:, 128:]
            else:
                xr = jnp.dot(lhs, br, preferred_element_type=jnp.float32)
                xi = jnp.dot(lhs, bi, preferred_element_type=jnp.float32)
            mr = (xr[: 2 * rows] - xi[2 * rows :]) * scale
            mi = (xi[: 2 * rows] + xr[2 * rows :]) * scale
            prod[j][0, at] = mr.reshape(2, rows, width)
            prod[j][1, at] = mi.reshape(2, rows, width)
            dr = a[0, at, :, here].reshape(2 * rows, width).astype(jnp.float32)
            di = a[1, at, :, here].reshape(2 * rows, width).astype(jnp.float32)
            terms = (mr * dr + mi * di, mr * di - mi * dr, mr * mr + mi * mi)
            for n, t in enumerate(terms):
                t = jnp.sum(t.reshape(-1, 8, width), axis=0)
                for w in range(0, width, 128):
                    sums[n] = sums[n] + t[:, w : w + 128]
    send_o(chunks - 1)

    line = [jnp.sum(u, axis=0, keepdims=True) for u in sums]
    value = jnp.concatenate(line + [jnp.zeros((5, 128), jnp.float32)], axis=0)
    stages = [
        (p, [pdev[1], pdev[3], pdev[2]], SIDE),
        (q, [qdev[1], qdev[3], qdev[2]], SIDE),
        (f, xdev[1:], freqs),
        (c, [{"shot": sib}], 2),
    ]
    for n, (me, to, size) in enumerate(stages):
        fit[n, me] = value

        def f_copy(i):
            here = fit.at[n, me]
            return remote(here, here, f_send.at[n, i], f_recv.at[n, i], to[i])

        def f_wait(i):
            there = fit.at[n, lax.rem(me - 1 - i + size, size)]
            return remote(there, there, f_send.at[n, i], f_recv.at[n, i], to[i])

        for i in range(size - 1):
            go(f_copy(i))
        for i in range(size - 1):
            f_wait(i).wait_recv()
        value = fit[n, 0]
        for i in range(1, size):
            value = value + fit[n, i]
    total = jnp.sum(value, axis=1, keepdims=True)
    count = float(freqs * order * order)
    den = total[2:3] / count + epsilon
    fit_re = total[0:1] / count / den
    fit_im = total[1:2] / count / den

    for j in range(chunks):
        for k in (0, 3, 1, 2):
            at = cols(q, ps[k], j)
            if k:
                o_copy(j, back[k]).wait_recv()
                mr, mi = own[0, :, at], own[1, :, at]
            else:
                mr, mi = prod[j][0, p], prod[j][1, p]
            mult_ref[0, :, at] = mr.astype(jnp.bfloat16)
            mult_ref[1, :, at] = mi.astype(jnp.bfloat16)
            dr, di = a[0, p, :, at].astype(jnp.float32), a[1, p, :, at].astype(jnp.float32)
            prim_ref[0, :, at] = (dr - (fit_re * mr - fit_im * mi)).astype(jnp.bfloat16)
            prim_ref[1, :, at] = (di - (fit_re * mi + fit_im * mr)).astype(jnp.bfloat16)
    for copy in sent:
        copy.wait_send()


def per_device(traces):
    rows, order = traces.shape[2], traces.shape[3]
    freqs = lax.axis_size("freq")
    widths = (256, 256, 256)
    chunks = len(widths)
    dma = pltpu.SemaphoreType.DMA
    out = jax.ShapeDtypeStruct((2, rows, order), jnp.bfloat16)
    shots = SIDE * SIDE * 2
    vmem = pl.BlockSpec(memory_space=pltpu.VMEM)
    mult, prim = pl.pallas_call(
        functools.partial(kernel, (freqs, rows, order, widths)),
        out_shape=(out, out),
        in_specs=[pl.BlockSpec(memory_space=pltpu.HBM)],
        out_specs=(vmem, vmem),
        scratch_shapes=[
            pltpu.VMEM((2, SIDE, rows, order), jnp.bfloat16),
            pltpu.VMEM((2, rows, order), jnp.float32),
            pltpu.VMEM((4, max(freqs, SIDE), 8, 128), jnp.float32),
            *[pltpu.VMEM((2, shots, rows, w), jnp.bfloat16) for w in widths],
            *[pltpu.VMEM((2, SIDE, rows, w), jnp.float32) for w in widths],
            dma, dma((chunks, SIDE)),
            dma((6,)), dma((6,)),
            dma((chunks, SIDE, SIDE)), dma((chunks, SIDE, SIDE)),
            dma((chunks, SIDE, SIDE)), dma((chunks, SIDE, SIDE)),
            dma((chunks, SIDE)), dma((chunks, SIDE)),
            dma((4, SIDE)), dma((4, SIDE)),
        ],
        compiler_params=pltpu.CompilerParams(
            collective_id=0, has_side_effects=True, vmem_limit_bytes=36 * 1024 * 1024
        ),
    )(pltpu.with_memory_space_constraint(traces.reshape(2, rows, order), pltpu.HBM))
    return mult.reshape(traces.shape), prim.reshape(traces.shape)


def solution(mesh):
    placed = P(None, "freq", "shot", None)
    return jax.shard_map(
        per_device,
        mesh=mesh,
        in_specs=(placed,),
        out_specs=(placed, placed),
        check_vma=False,
    )
```

```python
import functools
import math

import jax
import jax.numpy as jnp
from jax import lax
from jax.experimental import pallas as pl
from jax.experimental.pallas import tpu as pltpu
from jax.sharding import PartitionSpec as P

epsilon = 1e-06
SIDE = 4
MESH = pl.DeviceIdType.MESH
STEPS = (0, 1, -1, 2)


def kernel(
    dims, x_ref, mult_ref, prim_ref, a, b, prod, own, fit,
    load_sem, own_sem, a_send, a_recv, b_send, b_recv, d_send, d_recv, o_send, o_recv, f_send, f_recv,
):
    freqs, rows, order, widths = dims
    chunks = len(widths)
    starts = [sum(widths[:j]) for j in range(chunks)]
    block = order // SIDE
    scale = 1.0 / math.sqrt(order)
    f = lax.axis_index("freq")
    s = lax.axis_index("shot")
    c = lax.rem(s, 2)
    z = lax.rem(s // 2, SIDE)
    y = s // (2 * SIDE)
    p = z * (1 - c) + y * c
    q = y * (1 - c) + z * c

    def dev(qq, pp):
        return (1 - c) * ((qq * SIDE + pp) * 2) + c * ((pp * SIDE + qq) * 2 + 1)

    def turn(i, d):
        return lax.rem(i + d + SIDE, SIDE)

    ps = [turn(p, d) for d in STEPS]
    qs = [turn(q, d) for d in STEPS]
    pdev = [{"shot": dev(q, pp)} for pp in ps]
    qdev = [{"shot": dev(qq, p)} for qq in qs]
    xdev = [{"freq": lax.rem(f + i, freqs)} for i in range(freqs)]
    sib = {"shot": s + 1 - 2 * c}

    def lanes(j):
        return pl.ds(0, block) if j is None else pl.ds(starts[j], widths[j])

    def cols(qq, pp, j):
        at = lax.rem(qq + pp, SIDE) * block
        if j is None:
            return pl.ds(pl.multiple_of(at, 128), block)
        return pl.ds(pl.multiple_of(at + starts[j], 128), widths[j])

    def remote(src, dst, ss, rs, to):
        return pltpu.make_async_remote_copy(
            src_ref=src, dst_ref=dst, send_sem=ss, recv_sem=rs, device_id=to, device_id_type=MESH
        )

    def await_in(like, sem):
        remote(like, like, o_send, sem, sib).wait_recv()

    def await_out(like, sem):
        remote(like, like, sem, o_recv.at[0], sib).wait_send()

    load = pltpu.make_async_copy(x_ref, a.at[:, p], load_sem)
    load.start()

    barrier = pltpu.get_barrier_semaphore()
    near = pdev[1:] + qdev[1:] + [sib] + xdev[1:]
    for to in near:
        pl.semaphore_signal(barrier, inc=1, device_id=to, device_id_type=MESH)
    pl.semaphore_wait(barrier, len(near))
    load.wait()

    def send_a(n):
        h = (0, 1, 1, 0, 0, 1)[n]
        here = a.at[h, ps[(0, 0, 0, 0, 2, 1)[n]]]
        remote(here, here, a_send, a_recv.at[n], pdev[(1, 1, 2, 2, 1, 2)[n]]).start()

    def wait_a(n):
        await_in(a.at[(0, 1, 1, 0, 0, 1)[n], ps[(2, 2, 1, 1, 3, 3)[n]]], a_recv.at[n])

    def slot(r, j):
        return r if j is None else r + j

    def send_b(r, j=None):
        here = b.at[:, q * (1 - c) + ps[r] * c, ps[r] * (1 - c) + q * c, c, :, lanes(j)]
        for k in (3, 1, 2):
            remote(
                a.at[:, ps[r], :, cols(qs[k], p, j)], here, b_send, b_recv.at[slot(r, j)], qdev[k]
            ).start()
        pltpu.make_async_copy(a.at[:, ps[r], :, cols(q, p, j)], here, own_sem.at[slot(r, j)]).start()

    def pass_b(r, j=None):
        some = b.at[:, 0, :, 0, :, lanes(j)]
        mine = b.at[:, 0, 0, 0, :, lanes(j)]
        pltpu.make_async_copy(mine, mine, own_sem.at[slot(r, j)]).wait()
        await_in(b.at[:, 0, pl.ds(0, 3), 0, :, lanes(j)], b_recv.at[slot(r, j)])

        @pl.when(c == 0)
        def _():
            here = b.at[:, :, ps[r], 0, :, lanes(j)]
            remote(here, here, d_send, d_recv.at[slot(r, j)], sib).start()

        @pl.when(c == 1)
        def _():
            here = b.at[:, ps[r], :, 1, :, lanes(j)]
            remote(here, here, d_send, d_recv.at[slot(r, j)], sib).start()

        return some

    def wait_d(r, j=None):
        await_in(b.at[:, 0, :, 0, :, lanes(j)], d_recv.at[slot(r, j)])

    for n in (0, 2, 1, 3):
        send_a(n)
    send_b(0)
    for n in (0, 2):
        wait_a(n)
        send_a(n // 2 + 4)
    wait_a(1)
    send_b(2)
    wait_a(3)
    send_b(1)
    for n in (4, 5):
        wait_a(n)
    for j in range(chunks):
        send_b(3, j)
    for r in (0, 2, 1):
        pass_b(r)

    def send_o(j):
        for k in (3, 1, 2):
            remote(
                prod.at[:, ps[k], :, lanes(j)], own.at[:, :, cols(q, p, j)], o_send, o_recv.at[j], pdev[k]
            ).start()

    sums = [jnp.zeros((8, 128), jnp.float32) for _ in range(3)]
    depth = SIDE * SIDE * 2 * rows
    for j in range(chunks):
        width = widths[j]
        pass_b(3, j)
        if j == 0:
            for r in (0, 2, 1):
                wait_d(r)
        wait_d(3, j)
        here = cols(q, p, j)
        br = b[0, :, :, :, :, lanes(j)].reshape(depth, width)
        bi = b[1, :, :, :, :, lanes(j)].reshape(depth, width)
        for half in range(2):
            at = pl.ds(half * 2, 2)
            lhs = a[:, at].reshape(4 * rows, depth)
            if width == 128:
                x = jnp.dot(lhs, jnp.concatenate([br, bi], axis=1), preferred_element_type=jnp.float32)
                xr, xi = x[:, :128], x[:, 128:]
            else:
                xr = jnp.dot(lhs, br, preferred_element_type=jnp.float32)
                xi = jnp.dot(lhs, bi, preferred_element_type=jnp.float32)
            mr = (xr[: 2 * rows] - xi[2 * rows :]) * scale
            mi = (xi[: 2 * rows] + xr[2 * rows :]) * scale
            prod[0, at, :, lanes(j)] = mr.reshape(2, rows, width)
            prod[1, at, :, lanes(j)] = mi.reshape(2, rows, width)
            dr = a[0, at, :, here].reshape(2 * rows, width).astype(jnp.float32)
            di = a[1, at, :, here].reshape(2 * rows, width).astype(jnp.float32)
            terms = (mr * dr + mi * di, mr * di - mi * dr, mr * mr + mi * mi)
            for n, t in enumerate(terms):
                t = jnp.sum(t.reshape(-1, 8, width), axis=0)
                for w in range(0, width, 128):
                    sums[n] = sums[n] + t[:, w : w + 128]
        send_o(j)

    line = [jnp.sum(u, axis=0, keepdims=True) for u in sums]
    value = jnp.concatenate(line + [jnp.zeros((5, 128), jnp.float32)], axis=0)
    stages = [
        (c, [sib], 2),
        (f, xdev[1:], freqs),
        (q, [qdev[1], qdev[3], qdev[2]], SIDE),
        (p, [pdev[1], pdev[3], pdev[2]], SIDE),
    ]
    for n, (me, to, size) in enumerate(stages):
        fit[n, me] = value
        here = fit.at[n, me]
        for i in range(size - 1):
            remote(here, here, f_send.at[n], f_recv.at[n], to[i]).start()
        if size > 1:
            await_in(fit.at[n, pl.ds(0, size - 1)], f_recv.at[n])
        value = fit[n, 0]
        for i in range(1, size):
            value = value + fit[n, i]
    total = jnp.sum(value, axis=1, keepdims=True)
    count = float(freqs * order * order)
    den = total[2:3] / count + epsilon
    fit_re = total[0:1] / count / den
    fit_im = total[1:2] / count / den

    for j in range(chunks):
        for k in range(SIDE):
            at = cols(q, ps[k], j)
            if k:
                mr, mi = own[0, :, at], own[1, :, at]
            else:
                mr, mi = prod[0, p, :, lanes(j)], prod[1, p, :, lanes(j)]
            mult_ref[0, :, at] = mr.astype(jnp.bfloat16)
            mult_ref[1, :, at] = mi.astype(jnp.bfloat16)
            dr, di = a[0, p, :, at].astype(jnp.float32), a[1, p, :, at].astype(jnp.float32)
            prim_ref[0, :, at] = (dr - (fit_re * mr - fit_im * mi)).astype(jnp.bfloat16)
            prim_ref[1, :, at] = (di - (fit_re * mi + fit_im * mr)).astype(jnp.bfloat16)
            if k == 0:
                await_in(prod.at[:, pl.ds(0, 3), :, lanes(j)], o_recv.at[j])
    await_out(a.at[:, pl.ds(0, 3)], a_send)
    await_out(b.at[:, pl.ds(0, 3), :, 0], b_send)
    await_out(b.at[:, :, :, 0], d_send)
    await_out(prod.at[:, pl.ds(0, 3)], o_send)
    for n, (_, _, size) in enumerate(stages):
        if size > 1:
            await_out(fit.at[n, pl.ds(0, size - 1)], f_send.at[n])


def per_device(traces):
    rows, order = traces.shape[2], traces.shape[3]
    freqs = lax.axis_size("freq")
    block = order // SIDE
    widths = (256, 256, 256)
    chunks = len(widths)
    dma = pltpu.SemaphoreType.DMA
    out = jax.ShapeDtypeStruct((2, rows, order), jnp.bfloat16)
    vmem = pl.BlockSpec(memory_space=pltpu.VMEM)
    mult, prim = pl.pallas_call(
        functools.partial(kernel, (freqs, rows, order, widths)),
        out_shape=(out, out),
        in_specs=[pl.BlockSpec(memory_space=pltpu.HBM)],
        out_specs=(vmem, vmem),
        scratch_shapes=[
            pltpu.VMEM((2, SIDE, rows, order), jnp.bfloat16),
            pltpu.VMEM((2, SIDE, SIDE, 2, rows, block), jnp.bfloat16),
            pltpu.VMEM((2, SIDE, rows, block), jnp.float32),
            pltpu.VMEM((2, rows, order), jnp.float32),
            pltpu.VMEM((4, max(freqs, SIDE), 8, 128), jnp.float32),
            dma, dma((3 + chunks,)),
            dma, dma((6,)),
            dma, dma((3 + chunks,)),
            dma, dma((3 + chunks,)),
            dma, dma((chunks,)),
            dma((4,)), dma((4,)),
        ],
        compiler_params=pltpu.CompilerParams(
            collective_id=0, has_side_effects=True, vmem_limit_bytes=36 * 1024 * 1024
        ),
    )(pltpu.with_memory_space_constraint(traces.reshape(2, rows, order), pltpu.HBM))
    return mult.reshape(traces.shape), prim.reshape(traces.shape)


def solution(mesh):
    placed = P(None, "freq", "shot", None)
    return jax.shard_map(
        per_device,
        mesh=mesh,
        in_specs=(placed,),
        out_specs=(placed, placed),
        check_vma=False,
    )
```

```python
import functools
import math

import jax
import jax.numpy as jnp
from jax import lax
from jax.experimental import pallas as pl
from jax.experimental.pallas import tpu as pltpu
from jax.sharding import PartitionSpec as P

epsilon = 1e-06
SIDE = 4
MESH = pl.DeviceIdType.MESH
STEPS = (0, 1, -1, 2)


def kernel(
    dims, x_ref, mult_ref, prim_ref, a, b, prod, own, fit,
    load_sem, own_sem, a_send, a_recv, b_send, b_recv, d_send, d_recv, o_send, o_recv, f_send, f_recv,
):
    freqs, rows, order, widths, plan = dims
    pieces = [piece for part in plan for piece in part]
    chunks = len(widths)
    starts = [sum(widths[:j]) for j in range(chunks)]
    block = order // SIDE
    scale = 1.0 / math.sqrt(order)
    f = lax.axis_index("freq")
    s = lax.axis_index("shot")
    c = lax.rem(s, 2)
    z = lax.rem(s // 2, SIDE)
    y = s // (2 * SIDE)
    p = z * (1 - c) + y * c
    q = y * (1 - c) + z * c

    def dev(qq, pp):
        return (1 - c) * ((qq * SIDE + pp) * 2) + c * ((pp * SIDE + qq) * 2 + 1)

    def turn(i, d):
        return lax.rem(i + d + SIDE, SIDE)

    ps = [turn(p, d) for d in STEPS]
    qs = [turn(q, d) for d in STEPS]
    pdev = [{"shot": dev(q, pp)} for pp in ps]
    qdev = [{"shot": dev(qq, p)} for qq in qs]
    xdev = [{"freq": lax.rem(f + i, freqs)} for i in range(freqs)]
    sib = {"shot": s + 1 - 2 * c}

    ends = starts[1:] + [block]

    def lanes(i, j=None):
        j = i if j is None else j
        return pl.ds(starts[i], ends[j] - starts[i])

    def cols(qq, pp, i, j=None):
        j = i if j is None else j
        at = lax.rem(qq + pp, SIDE) * block + starts[i]
        return pl.ds(pl.multiple_of(at, 128), ends[j] - starts[i])

    def remote(src, dst, ss, rs, to):
        return pltpu.make_async_remote_copy(
            src_ref=src, dst_ref=dst, send_sem=ss, recv_sem=rs, device_id=to, device_id_type=MESH
        )

    def await_in(like, sem):
        remote(like, like, o_send, sem, sib).wait_recv()

    def await_out(like, sem):
        remote(like, like, sem, o_recv.at[0], sib).wait_send()

    load = pltpu.make_async_copy(x_ref, a.at[:, p], load_sem)
    load.start()

    barrier = pltpu.get_barrier_semaphore()
    near = pdev[1:] + qdev[1:] + [sib] + xdev[1:]
    for to in near:
        pl.semaphore_signal(barrier, inc=1, device_id=to, device_id_type=MESH)
    pl.semaphore_wait(barrier, len(near))
    load.wait()

    def send_a(n):
        h = (0, 1, 1, 0, 0, 1)[n]
        here = a.at[h, ps[(0, 0, 0, 0, 2, 1)[n]]]
        remote(here, here, a_send, a_recv.at[n], pdev[(1, 1, 2, 2, 1, 2)[n]]).start()

    def wait_a(n):
        await_in(a.at[(0, 1, 1, 0, 0, 1)[n], ps[(2, 2, 1, 1, 3, 3)[n]]], a_recv.at[n])

    def send_b(piece):
        n = pieces.index(piece)
        r, lo, hi = piece
        here = b.at[:, q * (1 - c) + ps[r] * c, ps[r] * (1 - c) + q * c, c, :, lanes(lo, hi)]
        for k in (1, 2, 3):
            remote(a.at[:, ps[r], :, cols(qs[k], p, lo, hi)], here, b_send, b_recv.at[n], qdev[k]).start()
        pltpu.make_async_copy(a.at[:, ps[r], :, cols(q, p, lo, hi)], here, own_sem.at[n]).start()

    def pass_b(piece):
        n = pieces.index(piece)
        r, lo, hi = piece
        mine = b.at[:, 0, 0, 0, :, lanes(lo, hi)]
        pltpu.make_async_copy(mine, mine, own_sem.at[n]).wait()
        await_in(b.at[:, 0, pl.ds(0, 3), 0, :, lanes(lo, hi)], b_recv.at[n])

        @pl.when(c == 0)
        def _():
            here = b.at[:, :, ps[r], 0, :, lanes(lo, hi)]
            remote(here, here, d_send, d_recv.at[n], sib).start()

        @pl.when(c == 1)
        def _():
            here = b.at[:, ps[r], :, 1, :, lanes(lo, hi)]
            remote(here, here, d_send, d_recv.at[n], sib).start()

    def wait_d(piece):
        await_in(b.at[:, 0, :, 0, :, lanes(*piece[1:])], d_recv.at[pieces.index(piece)])

    for n in (0, 2, 1, 3):
        send_a(n)
    for piece in plan[0]:
        send_b(piece)
    for n in (0, 2):
        wait_a(n)
        send_a(n // 2 + 4)
    for n in (1, 3):
        wait_a(n)
    for piece in plan[1]:
        send_b(piece)
    for n in (4, 5):
        wait_a(n)
    for piece in plan[2]:
        send_b(piece)

    def send_o(j):
        for k in (3, 1, 2):
            remote(
                prod.at[:, ps[k], :, lanes(j)], own.at[:, :, cols(q, p, j)], o_send, o_recv.at[j], pdev[k]
            ).start()

    sums = [jnp.zeros((8, 128), jnp.float32) for _ in range(3)]
    depth = SIDE * SIDE * 2 * rows
    passed = 0
    for j in range(chunks):
        width = widths[j]
        last = max(n for n, (r, lo, hi) in enumerate(pieces) if lo <= j)
        for piece in pieces[passed : last + 1]:
            pass_b(piece)
        for piece in pieces[passed : last + 1]:
            wait_d(piece)
        passed = max(passed, last + 1)
        here = cols(q, p, j)
        br = b[0, :, :, :, :, lanes(j)].reshape(depth, width)
        bi = b[1, :, :, :, :, lanes(j)].reshape(depth, width)
        for half in range(2):
            at = pl.ds(half * 2, 2)
            lhs = a[:, at].reshape(4 * rows, depth)
            if width == 128:
                x = jnp.dot(lhs, jnp.concatenate([br, bi], axis=1), preferred_element_type=jnp.float32)
                xr, xi = x[:, :128], x[:, 128:]
            else:
                xr = jnp.dot(lhs, br, preferred_element_type=jnp.float32)
                xi = jnp.dot(lhs, bi, preferred_element_type=jnp.float32)
            mr = (xr[: 2 * rows] - xi[2 * rows :]) * scale
            mi = (xi[: 2 * rows] + xr[2 * rows :]) * scale
            prod[0, at, :, lanes(j)] = mr.reshape(2, rows, width)
            prod[1, at, :, lanes(j)] = mi.reshape(2, rows, width)
            dr = a[0, at, :, here].reshape(2 * rows, width).astype(jnp.float32)
            di = a[1, at, :, here].reshape(2 * rows, width).astype(jnp.float32)
            terms = (mr * dr + mi * di, mr * di - mi * dr, mr * mr + mi * mi)
            for n, t in enumerate(terms):
                t = jnp.sum(t.reshape(-1, 8, width), axis=0)
                for w in range(0, width, 128):
                    sums[n] = sums[n] + t[:, w : w + 128]
        send_o(j)

    line = [jnp.sum(u, axis=0, keepdims=True) for u in sums]
    value = jnp.concatenate(line + [jnp.zeros((5, 128), jnp.float32)], axis=0)
    stages = [
        (c, [sib], 2),
        (f, xdev[1:], freqs),
        (q, [qdev[1], qdev[3], qdev[2]], SIDE),
        (p, [pdev[1], pdev[3], pdev[2]], SIDE),
    ]
    for n, (me, to, size) in enumerate(stages):
        fit[n, me] = value
        here = fit.at[n, me]
        for i in range(size - 1):
            remote(here, here, f_send.at[n], f_recv.at[n], to[i]).start()
        if size > 1:
            await_in(fit.at[n, pl.ds(0, size - 1)], f_recv.at[n])
        value = fit[n, 0]
        for i in range(1, size):
            value = value + fit[n, i]
    total = jnp.sum(value, axis=1, keepdims=True)
    count = float(freqs * order * order)
    den = total[2:3] / count + epsilon
    fit_re = total[0:1] / count / den
    fit_im = total[1:2] / count / den

    for j in range(chunks):
        for k in range(SIDE):
            at = cols(q, ps[k], j)
            if k:
                mr, mi = own[0, :, at], own[1, :, at]
            else:
                mr, mi = prod[0, p, :, lanes(j)], prod[1, p, :, lanes(j)]
            mult_ref[0, :, at] = mr.astype(jnp.bfloat16)
            mult_ref[1, :, at] = mi.astype(jnp.bfloat16)
            dr, di = a[0, p, :, at].astype(jnp.float32), a[1, p, :, at].astype(jnp.float32)
            prim_ref[0, :, at] = (dr - (fit_re * mr - fit_im * mi)).astype(jnp.bfloat16)
            prim_ref[1, :, at] = (di - (fit_re * mi + fit_im * mr)).astype(jnp.bfloat16)
            if k == 0:
                await_in(prod.at[:, pl.ds(0, 3), :, lanes(j)], o_recv.at[j])
    await_out(a.at[:, pl.ds(0, 3)], a_send)
    await_out(b.at[:, pl.ds(0, 3), :, 0], b_send)
    await_out(b.at[:, :, :, 0], d_send)
    await_out(prod.at[:, pl.ds(0, 3)], o_send)
    for n, (_, _, size) in enumerate(stages):
        if size > 1:
            await_out(fit.at[n, pl.ds(0, size - 1)], f_send.at[n])


def per_device(traces):
    rows, order = traces.shape[2], traces.shape[3]
    freqs = lax.axis_size("freq")
    block = order // SIDE
    widths = (256, 256, 256)
    chunks = len(widths)
    plan = ((), ((0, 0, 2), (2, 0, 1), (1, 0, 1)), ((3, 0, 0), (3, 1, 1), (2, 2, 2), (1, 2, 2), (3, 2, 2)))
    pieces = sum(len(part) for part in plan)
    dma = pltpu.SemaphoreType.DMA
    out = jax.ShapeDtypeStruct((2, rows, order), jnp.bfloat16)
    vmem = pl.BlockSpec(memory_space=pltpu.VMEM)
    mult, prim = pl.pallas_call(
        functools.partial(kernel, (freqs, rows, order, widths, plan)),
        out_shape=(out, out),
        in_specs=[pl.BlockSpec(memory_space=pltpu.HBM)],
        out_specs=(vmem, vmem),
        scratch_shapes=[
            pltpu.VMEM((2, SIDE, rows, order), jnp.bfloat16),
            pltpu.VMEM((2, SIDE, SIDE, 2, rows, block), jnp.bfloat16),
            pltpu.VMEM((2, SIDE, rows, block), jnp.float32),
            pltpu.VMEM((2, rows, order), jnp.float32),
            pltpu.VMEM((4, max(freqs, SIDE), 8, 128), jnp.float32),
            dma, dma((pieces,)),
            dma, dma((6,)),
            dma, dma((pieces,)),
            dma, dma((pieces,)),
            dma, dma((chunks,)),
            dma((4,)), dma((4,)),
        ],
        compiler_params=pltpu.CompilerParams(
            collective_id=0, has_side_effects=True, vmem_limit_bytes=36 * 1024 * 1024
        ),
    )(pltpu.with_memory_space_constraint(traces.reshape(2, rows, order), pltpu.HBM))
    return mult.reshape(traces.shape), prim.reshape(traces.shape)


def solution(mesh):
    placed = P(None, "freq", "shot", None)
    return jax.shard_map(
        per_device,
        mesh=mesh,
        in_specs=(placed,),
        out_specs=(placed, placed),
        check_vma=False,
    )
```

```python
import functools
import math

import jax
import jax.numpy as jnp
from jax import lax
from jax.experimental import pallas as pl
from jax.experimental.pallas import tpu as pltpu
from jax.sharding import PartitionSpec as P

epsilon = 1e-06
SIDE = 4
MESH = pl.DeviceIdType.MESH
STEPS = (0, 1, -1, 2)


def kernel(
    dims, x_ref, own, fit_ref, a, b, prod, fit, plane,
    load_sem, own_sem, a_send, a_recv, b_send, b_recv, d_send, d_recv, o_send, o_recv, f_send, f_recv,
):
    freqs, rows, order, widths, plan = dims
    pieces = [piece for part in plan for piece in part]
    chunks = len(widths)
    starts = [sum(widths[:j]) for j in range(chunks)]
    block = order // SIDE
    scale = 1.0 / math.sqrt(order)
    f = lax.axis_index("freq")
    s = lax.axis_index("shot")
    c = lax.rem(s, 2)
    z = lax.rem(s // 2, SIDE)
    y = s // (2 * SIDE)
    p = z * (1 - c) + y * c
    q = y * (1 - c) + z * c

    def dev(qq, pp):
        return (1 - c) * ((qq * SIDE + pp) * 2) + c * ((pp * SIDE + qq) * 2 + 1)

    def turn(i, d):
        return lax.rem(i + d + SIDE, SIDE)

    ps = [turn(p, d) for d in STEPS]
    qs = [turn(q, d) for d in STEPS]
    pdev = [{"shot": dev(q, pp)} for pp in ps]
    qdev = [{"shot": dev(qq, p)} for qq in qs]
    sib = {"shot": s + 1 - 2 * c}

    ends = starts[1:] + [block]

    def lanes(i, j=None):
        j = i if j is None else j
        return pl.ds(starts[i], ends[j] - starts[i])

    def cols(qq, pp, i, j=None):
        j = i if j is None else j
        at = lax.rem(qq + pp, SIDE) * block + starts[i]
        return pl.ds(pl.multiple_of(at, 128), ends[j] - starts[i])

    def remote(src, dst, ss, rs, to):
        return pltpu.make_async_remote_copy(
            src_ref=src, dst_ref=dst, send_sem=ss, recv_sem=rs, device_id=to, device_id_type=MESH
        )

    def await_in(like, sem):
        remote(like, like, o_send, sem, sib).wait_recv()

    def await_out(like, sem):
        remote(like, like, sem, o_recv.at[0], sib).wait_send()

    load = pltpu.make_async_copy(x_ref, a.at[:, p], load_sem)
    load.start()

    barrier = pltpu.get_barrier_semaphore()
    ids = [(i, k) for i in range(freqs) for k in (0, 1) if i or k]
    fdev = [{"freq": lax.rem(f + i, freqs), "shot": s + k * (1 - 2 * c)} for i, k in ids]
    near = pdev[1:] + qdev[1:] + fdev
    for to in near:
        pl.semaphore_signal(barrier, inc=1, device_id=to, device_id_type=MESH)
    pl.semaphore_wait(barrier, len(near))
    load.wait()

    def send_a(n):
        h = (0, 1, 1, 0, 0, 1)[n]
        here = a.at[h, ps[(0, 0, 0, 0, 2, 1)[n]]]
        remote(here, here, a_send, a_recv.at[n], pdev[(1, 1, 2, 2, 1, 2)[n]]).start()

    def wait_a(n):
        await_in(a.at[(0, 1, 1, 0, 0, 1)[n], ps[(2, 2, 1, 1, 3, 3)[n]]], a_recv.at[n])

    def send_b(piece):
        n = pieces.index(piece)
        r, lo, hi = piece
        here = b.at[:, q * (1 - c) + ps[r] * c, ps[r] * (1 - c) + q * c, c, :, lanes(lo, hi)]
        for k in (1, 2, 3):
            remote(a.at[:, ps[r], :, cols(qs[k], p, lo, hi)], here, b_send, b_recv.at[n], qdev[k]).start()
        pltpu.make_async_copy(a.at[:, ps[r], :, cols(q, p, lo, hi)], here, own_sem.at[n]).start()

    def pass_b(piece):
        n = pieces.index(piece)
        r, lo, hi = piece
        mine = b.at[:, 0, 0, 0, :, lanes(lo, hi)]
        pltpu.make_async_copy(mine, mine, own_sem.at[n]).wait()
        await_in(b.at[:, 0, pl.ds(0, 3), 0, :, lanes(lo, hi)], b_recv.at[n])

        @pl.when(c == 0)
        def _():
            here = b.at[:, :, ps[r], 0, :, lanes(lo, hi)]
            remote(here, here, d_send, d_recv.at[n], sib).start()

        @pl.when(c == 1)
        def _():
            here = b.at[:, ps[r], :, 1, :, lanes(lo, hi)]
            remote(here, here, d_send, d_recv.at[n], sib).start()

    def wait_d(piece):
        await_in(b.at[:, 0, :, 0, :, lanes(*piece[1:])], d_recv.at[pieces.index(piece)])

    for n in (0, 2, 1, 3):
        send_a(n)
    for piece in plan[0]:
        send_b(piece)
    for n in (0, 2):
        wait_a(n)
        send_a(n // 2 + 4)
    for n in (1, 3):
        wait_a(n)
    for piece in plan[1]:
        send_b(piece)
    for n in (4, 5):
        wait_a(n)
    for piece in plan[2]:
        send_b(piece)

    def send_o(j):
        for k in (3, 1, 2):
            remote(
                prod.at[:, ps[k], :, lanes(j)], own.at[:, :, cols(q, p, j)], o_send, o_recv.at[j], pdev[k]
            ).start()

    sums = [jnp.zeros((8, 128), jnp.float32) for _ in range(3)]
    depth = SIDE * SIDE * 2 * rows
    passed = 0
    for j in range(chunks):
        width = widths[j]
        last = max(n for n, (r, lo, hi) in enumerate(pieces) if lo <= j)
        for piece in pieces[passed : last + 1]:
            pass_b(piece)
        for piece in pieces[passed : last + 1]:
            wait_d(piece)
        passed = max(passed, last + 1)
        here = cols(q, p, j)
        br = b[0, :, :, :, :, lanes(j)].reshape(depth, width)
        bi = b[1, :, :, :, :, lanes(j)].reshape(depth, width)
        for half in range(2):
            at = pl.ds(half * 2, 2)
            lhs = a[:, at].reshape(4 * rows, depth)
            if width == 128:
                x = jnp.dot(lhs, jnp.concatenate([br, bi], axis=1), preferred_element_type=jnp.float32)
                xr, xi = x[:, :128], x[:, 128:]
            else:
                xr = jnp.dot(lhs, br, preferred_element_type=jnp.float32)
                xi = jnp.dot(lhs, bi, preferred_element_type=jnp.float32)
            mr = (xr[: 2 * rows] - xi[2 * rows :]) * scale
            mi = (xi[: 2 * rows] + xr[2 * rows :]) * scale
            prod[0, at, :, lanes(j)] = mr.reshape(2, rows, width)
            prod[1, at, :, lanes(j)] = mi.reshape(2, rows, width)
            dr = a[0, at, :, here].reshape(2 * rows, width).astype(jnp.float32)
            di = a[1, at, :, here].reshape(2 * rows, width).astype(jnp.float32)
            terms = (mr * dr + mi * di, mr * di - mi * dr, mr * mr + mi * mi)
            for n, t in enumerate(terms):
                t = jnp.sum(t.reshape(-1, 8, width), axis=0)
                for w in range(0, width, 128):
                    sums[n] = sums[n] + t[:, w : w + 128]
        send_o(j)

    line = [jnp.sum(u, axis=0, keepdims=True) for u in sums]
    mine = fit.at[f * 2 + c]
    mine[...] = jnp.concatenate(line + [jnp.zeros((5, 128), jnp.float32)], axis=0)
    for to in fdev:
        remote(mine, mine, f_send.at[0], f_recv.at[0], to).start()
    for j in range(chunks):
        own[:, :, cols(q, p, j)] = prod[:, p, :, lanes(j)]
    await_in(fit.at[pl.ds(0, len(fdev))], f_recv.at[0])
    here = plane.at[q * SIDE + p]
    here[...] = jnp.sum(fit[...], axis=0)
    others = [(i, k) for i in range(SIDE) for k in range(SIDE) if i or k]
    for i, k in others:
        remote(here, here, f_send.at[1], f_recv.at[1], {"shot": dev(qs[i], ps[k])}).start()
    for j in range(chunks):
        await_in(prod.at[:, pl.ds(0, 3), :, lanes(j)], o_recv.at[j])
    await_in(plane.at[pl.ds(0, len(others))], f_recv.at[1])
    fit_ref[...] = jnp.sum(plane[...], axis=0)
    await_out(a.at[:, pl.ds(0, 3)], a_send)
    await_out(b.at[:, pl.ds(0, 3), :, 0], b_send)
    await_out(b.at[:, :, :, 0], d_send)
    await_out(prod.at[:, pl.ds(0, 3)], o_send)
    await_out(fit.at[pl.ds(0, len(fdev))], f_send.at[0])
    await_out(plane.at[pl.ds(0, len(others))], f_send.at[1])


def finish(count, own, fit, x, mult_ref, prim_ref, mult, prim, m_sem, p_sem):
    total = jnp.sum(fit[...], axis=1, keepdims=True)
    den = total[2:3] / count + epsilon
    fit_re = total[0:1] / count / den
    fit_im = total[1:2] / count / den
    rows = own.shape[1]
    copies = []
    for n in range(rows // 32):
        at = pl.ds(n * 32, 32)
        mr, mi = own[0, at], own[1, at]
        mult[0, at] = mr.astype(jnp.bfloat16)
        mult[1, at] = mi.astype(jnp.bfloat16)
        copies.append(pltpu.make_async_copy(mult.at[:, at], mult_ref.at[:, at], m_sem.at[n]))
        copies[-1].start()
        dr, di = x[0, at].astype(jnp.float32), x[1, at].astype(jnp.float32)
        prim[0, at] = (dr - (fit_re * mr - fit_im * mi)).astype(jnp.bfloat16)
        prim[1, at] = (di - (fit_re * mi + fit_im * mr)).astype(jnp.bfloat16)
        copies.append(pltpu.make_async_copy(prim.at[:, at], prim_ref.at[:, at], p_sem.at[n]))
        copies[-1].start()
    for copy in copies:
        copy.wait()


def per_device(traces):
    rows, order = traces.shape[2], traces.shape[3]
    freqs = lax.axis_size("freq")
    block = order // SIDE
    widths = (256, 256, 256)
    chunks = len(widths)
    plan = ((), ((0, 0, 2), (2, 0, 1), (1, 0, 1)), ((3, 0, 0), (3, 1, 1), (2, 2, 2), (1, 2, 2), (3, 2, 2)))
    pieces = sum(len(part) for part in plan)
    dma = pltpu.SemaphoreType.DMA
    out = jax.ShapeDtypeStruct((2, rows, order), jnp.bfloat16)
    vmem = pl.BlockSpec(memory_space=pltpu.VMEM)
    x = traces.reshape(2, rows, order)
    anywhere = pl.BlockSpec(memory_space=pl.ANY)
    own, fit = pl.pallas_call(
        functools.partial(kernel, (freqs, rows, order, widths, plan)),
        out_shape=(
            jax.ShapeDtypeStruct((2, rows, order), jnp.float32),
            jax.ShapeDtypeStruct((8, 128), jnp.float32),
        ),
        in_specs=[pl.BlockSpec(memory_space=pltpu.HBM)],
        out_specs=(vmem, vmem),
        scratch_shapes=[
            pltpu.VMEM((2, SIDE, rows, order), jnp.bfloat16),
            pltpu.VMEM((2, SIDE, SIDE, 2, rows, block), jnp.bfloat16),
            pltpu.VMEM((2, SIDE, rows, block), jnp.float32),
            pltpu.VMEM((freqs * 2, 8, 128), jnp.float32),
            pltpu.VMEM((SIDE * SIDE, 8, 128), jnp.float32),
            dma, dma((pieces,)),
            dma, dma((6,)),
            dma, dma((pieces,)),
            dma, dma((pieces,)),
            dma, dma((chunks,)),
            dma((2,)), dma((2,)),
        ],
        compiler_params=pltpu.CompilerParams(
            collective_id=0, has_side_effects=True, vmem_limit_bytes=36 * 1024 * 1024
        ),
    )(pltpu.with_memory_space_constraint(x, pltpu.HBM))
    mult, prim = pl.pallas_call(
        functools.partial(finish, float(freqs * order * order)),
        out_shape=(out, out),
        in_specs=[vmem, vmem, vmem],
        out_specs=(anywhere, anywhere),
        scratch_shapes=[
            pltpu.VMEM((2, rows, order), jnp.bfloat16),
            pltpu.VMEM((2, rows, order), jnp.bfloat16),
            dma((rows // 32,)), dma((rows // 32,)),
        ],
        compiler_params=pltpu.CompilerParams(vmem_limit_bytes=16 * 1024 * 1024),
    )(own, fit, x)
    return mult.reshape(traces.shape), prim.reshape(traces.shape)


def solution(mesh):
    placed = P(None, "freq", "shot", None)
    return jax.shard_map(
        per_device,
        mesh=mesh,
        in_specs=(placed,),
        out_specs=(placed, placed),
        check_vma=False,
    )
```

```python
import functools
import math

import jax
import jax.numpy as jnp
from jax import lax
from jax.experimental import pallas as pl
from jax.experimental.pallas import tpu as pltpu
from jax.sharding import PartitionSpec as P

epsilon = 1e-06
SIDE = 4
MESH = pl.DeviceIdType.MESH
STEPS = (0, 1, -1, 2)


def kernel(
    dims, x_ref, own, fit_ref, a, b, prod, fit, plane,
    load_sem, own_sem, a_send, a_recv, b_send, b_recv, d_send, d_recv, o_send, o_recv, f_send, f_recv,
):
    freqs, rows, order, widths, plan = dims
    pieces = [piece for part in plan for piece in part]
    chunks = len(widths)
    starts = [sum(widths[:j]) for j in range(chunks)]
    block = order // SIDE
    scale = 1.0 / math.sqrt(order)
    f = lax.axis_index("freq")
    s = lax.axis_index("shot")
    c = lax.rem(s, 2)
    z = lax.rem(s // 2, SIDE)
    y = s // (2 * SIDE)
    p = z * (1 - c) + y * c
    q = y * (1 - c) + z * c

    def dev(qq, pp):
        return (1 - c) * ((qq * SIDE + pp) * 2) + c * ((pp * SIDE + qq) * 2 + 1)

    def turn(i, d):
        return lax.rem(i + d + SIDE, SIDE)

    ps = [turn(p, d) for d in STEPS]
    qs = [turn(q, d) for d in STEPS]
    pdev = [{"shot": dev(q, pp)} for pp in ps]
    qdev = [{"shot": dev(qq, p)} for qq in qs]
    sib = {"shot": s + 1 - 2 * c}

    ends = starts[1:] + [block]

    def lanes(i, j=None):
        j = i if j is None else j
        return pl.ds(starts[i], ends[j] - starts[i])

    def cols(qq, pp, i, j=None):
        j = i if j is None else j
        at = lax.rem(qq + pp, SIDE) * block + starts[i]
        return pl.ds(pl.multiple_of(at, 128), ends[j] - starts[i])

    def remote(src, dst, ss, rs, to):
        return pltpu.make_async_remote_copy(
            src_ref=src, dst_ref=dst, send_sem=ss, recv_sem=rs, device_id=to, device_id_type=MESH
        )

    def await_in(like, sem):
        remote(like, like, o_send, sem, sib).wait_recv()

    def await_out(like, sem):
        remote(like, like, sem, o_recv.at[0], sib).wait_send()

    load = pltpu.make_async_copy(x_ref, a.at[:, p], load_sem)
    load.start()

    barrier = pltpu.get_barrier_semaphore()
    ids = [(i, k) for i in range(freqs) for k in (0, 1) if i or k]
    fdev = [{"freq": lax.rem(f + i, freqs), "shot": s + k * (1 - 2 * c)} for i, k in ids]
    near = pdev[1:] + qdev[1:] + fdev
    for to in near:
        pl.semaphore_signal(barrier, inc=1, device_id=to, device_id_type=MESH)
    pl.semaphore_wait(barrier, len(near))
    load.wait()

    def send_a(n):
        h = (0, 1, 1, 0, 0, 1)[n]
        here = a.at[h, ps[(0, 0, 0, 0, 2, 1)[n]]]
        remote(here, here, a_send, a_recv.at[n], pdev[(1, 1, 2, 2, 1, 2)[n]]).start()

    def wait_a(n):
        await_in(a.at[(0, 1, 1, 0, 0, 1)[n], ps[(2, 2, 1, 1, 3, 3)[n]]], a_recv.at[n])

    def send_b(piece):
        n = pieces.index(piece)
        r, lo, hi = piece
        here = b.at[:, q * (1 - c) + ps[r] * c, ps[r] * (1 - c) + q * c, c, :, lanes(lo, hi)]
        for k in (1, 2, 3):
            remote(a.at[:, ps[r], :, cols(qs[k], p, lo, hi)], here, b_send, b_recv.at[n], qdev[k]).start()
        pltpu.make_async_copy(a.at[:, ps[r], :, cols(q, p, lo, hi)], here, own_sem.at[n]).start()

    def pass_b(piece):
        n = pieces.index(piece)
        r, lo, hi = piece
        mine = b.at[:, 0, 0, 0, :, lanes(lo, hi)]
        pltpu.make_async_copy(mine, mine, own_sem.at[n]).wait()
        await_in(b.at[:, 0, pl.ds(0, 3), 0, :, lanes(lo, hi)], b_recv.at[n])

        @pl.when(c == 0)
        def _():
            here = b.at[:, :, ps[r], 0, :, lanes(lo, hi)]
            remote(here, here, d_send, d_recv.at[n], sib).start()

        @pl.when(c == 1)
        def _():
            here = b.at[:, ps[r], :, 1, :, lanes(lo, hi)]
            remote(here, here, d_send, d_recv.at[n], sib).start()

    def wait_d(piece):
        await_in(b.at[:, 0, :, 0, :, lanes(*piece[1:])], d_recv.at[pieces.index(piece)])

    for n in (0, 2, 1, 3):
        send_a(n)
    for piece in plan[0]:
        send_b(piece)
    for n in (0, 2):
        wait_a(n)
        send_a(n // 2 + 4)
    for n in (1, 3):
        wait_a(n)
    for piece in plan[1]:
        send_b(piece)
    for n in (4, 5):
        wait_a(n)
    for piece in plan[2]:
        send_b(piece)

    def send_o(j):
        for k in (3, 1, 2):
            remote(
                prod.at[:, ps[k], :, lanes(j)], own.at[:, :, cols(q, p, j)], o_send, o_recv.at[j], pdev[k]
            ).start()

    sums = [jnp.zeros((8, 128), jnp.float32) for _ in range(3)]
    depth = SIDE * SIDE * 2 * rows
    passed = 0
    for j in range(chunks):
        width = widths[j]
        last = max(n for n, (r, lo, hi) in enumerate(pieces) if lo <= j)
        for piece in pieces[passed : last + 1]:
            pass_b(piece)
        for piece in pieces[passed : last + 1]:
            wait_d(piece)
        passed = max(passed, last + 1)
        here = cols(q, p, j)
        br = b[0, :, :, :, :, lanes(j)].reshape(depth, width)
        bi = b[1, :, :, :, :, lanes(j)].reshape(depth, width)
        for half in range(2):
            at = pl.ds(half * 2, 2)
            lhs = a[:, at].reshape(4 * rows, depth)
            if width == 128:
                x = jnp.dot(lhs, jnp.concatenate([br, bi], axis=1), preferred_element_type=jnp.float32)
                xr, xi = x[:, :128], x[:, 128:]
            else:
                xr = jnp.dot(lhs, br, preferred_element_type=jnp.float32)
                xi = jnp.dot(lhs, bi, preferred_element_type=jnp.float32)
            mr = (xr[: 2 * rows] - xi[2 * rows :]) * scale
            mi = (xi[: 2 * rows] + xr[2 * rows :]) * scale
            prod[0, at, :, lanes(j)] = mr.reshape(2, rows, width)
            prod[1, at, :, lanes(j)] = mi.reshape(2, rows, width)
            dr = a[0, at, :, here].reshape(2 * rows, width).astype(jnp.float32)
            di = a[1, at, :, here].reshape(2 * rows, width).astype(jnp.float32)
            terms = (mr * dr + mi * di, mr * di - mi * dr, mr * mr + mi * mi)
            for n, t in enumerate(terms):
                t = jnp.sum(t.reshape(-1, 8, width), axis=0)
                for w in range(0, width, 128):
                    sums[n] = sums[n] + t[:, w : w + 128]
        if j < chunks - 1:
            send_o(j)

    line = [jnp.sum(u, axis=0, keepdims=True) for u in sums]
    mine = fit.at[f * 2 + c]
    mine[...] = jnp.concatenate(line + [jnp.zeros((5, 128), jnp.float32)], axis=0)
    for to in fdev:
        remote(mine, mine, f_send.at[0], f_recv.at[0], to).start()
    send_o(chunks - 1)
    for j in range(chunks):
        own[:, :, cols(q, p, j)] = prod[:, p, :, lanes(j)]
    await_in(fit.at[pl.ds(0, len(fdev))], f_recv.at[0])
    here = plane.at[q * SIDE + p]
    here[...] = jnp.sum(fit[...], axis=0)
    others = [(i, k) for i in range(SIDE) for k in range(SIDE) if i or k]
    for i, k in others:
        remote(here, here, f_send.at[1], f_recv.at[1], {"shot": dev(qs[i], ps[k])}).start()
    for j in range(chunks):
        await_in(prod.at[:, pl.ds(0, 3), :, lanes(j)], o_recv.at[j])
    await_in(plane.at[pl.ds(0, len(others))], f_recv.at[1])
    fit_ref[...] = jnp.sum(plane[...], axis=0)
    await_out(a.at[:, pl.ds(0, 3)], a_send)
    await_out(b.at[:, pl.ds(0, 3), :, 0], b_send)
    await_out(b.at[:, :, :, 0], d_send)
    await_out(prod.at[:, pl.ds(0, 3)], o_send)
    await_out(fit.at[pl.ds(0, len(fdev))], f_send.at[0])
    await_out(plane.at[pl.ds(0, len(others))], f_send.at[1])


def finish(count, own, fit, x, mult_ref, prim_ref, mult, prim, m_sem, p_sem):
    total = jnp.sum(fit[...], axis=1, keepdims=True)
    den = total[2:3] / count + epsilon
    fit_re = total[0:1] / count / den
    fit_im = total[1:2] / count / den
    rows = own.shape[1]
    copies = []
    for n in range(rows // 16):
        at = pl.ds(n * 16, 16)
        mr, mi = own[0, at], own[1, at]
        mult[0, at] = mr.astype(jnp.bfloat16)
        mult[1, at] = mi.astype(jnp.bfloat16)
        copies.append(pltpu.make_async_copy(mult.at[:, at], mult_ref.at[:, at], m_sem.at[n]))
        copies[-1].start()
        dr, di = x[0, at].astype(jnp.float32), x[1, at].astype(jnp.float32)
        prim[0, at] = (dr - (fit_re * mr - fit_im * mi)).astype(jnp.bfloat16)
        prim[1, at] = (di - (fit_re * mi + fit_im * mr)).astype(jnp.bfloat16)
        copies.append(pltpu.make_async_copy(prim.at[:, at], prim_ref.at[:, at], p_sem.at[n]))
        copies[-1].start()
    for copy in copies:
        copy.wait()


def per_device(traces):
    rows, order = traces.shape[2], traces.shape[3]
    freqs = lax.axis_size("freq")
    block = order // SIDE
    widths = (256, 256, 256)
    chunks = len(widths)
    plan = ((), ((0, 0, 2), (2, 0, 1), (1, 0, 1)), ((3, 0, 0), (3, 1, 1), (2, 2, 2), (1, 2, 2), (3, 2, 2)))
    pieces = sum(len(part) for part in plan)
    dma = pltpu.SemaphoreType.DMA
    out = jax.ShapeDtypeStruct((2, rows, order), jnp.bfloat16)
    vmem = pl.BlockSpec(memory_space=pltpu.VMEM)
    x = traces.reshape(2, rows, order)
    anywhere = pl.BlockSpec(memory_space=pl.ANY)
    own, fit = pl.pallas_call(
        functools.partial(kernel, (freqs, rows, order, widths, plan)),
        out_shape=(
            jax.ShapeDtypeStruct((2, rows, order), jnp.float32),
            jax.ShapeDtypeStruct((8, 128), jnp.float32),
        ),
        in_specs=[pl.BlockSpec(memory_space=pltpu.HBM)],
        out_specs=(vmem, vmem),
        scratch_shapes=[
            pltpu.VMEM((2, SIDE, rows, order), jnp.bfloat16),
            pltpu.VMEM((2, SIDE, SIDE, 2, rows, block), jnp.bfloat16),
            pltpu.VMEM((2, SIDE, rows, block), jnp.float32),
            pltpu.VMEM((freqs * 2, 8, 128), jnp.float32),
            pltpu.VMEM((SIDE * SIDE, 8, 128), jnp.float32),
            dma, dma((pieces,)),
            dma, dma((6,)),
            dma, dma((pieces,)),
            dma, dma((pieces,)),
            dma, dma((chunks,)),
            dma((2,)), dma((2,)),
        ],
        compiler_params=pltpu.CompilerParams(
            collective_id=0, has_side_effects=True, vmem_limit_bytes=36 * 1024 * 1024
        ),
    )(pltpu.with_memory_space_constraint(x, pltpu.HBM))
    mult, prim = pl.pallas_call(
        functools.partial(finish, float(freqs * order * order)),
        out_shape=(out, out),
        in_specs=[vmem, vmem, vmem],
        out_specs=(anywhere, anywhere),
        scratch_shapes=[
            pltpu.VMEM((2, rows, order), jnp.bfloat16),
            pltpu.VMEM((2, rows, order), jnp.bfloat16),
            dma((rows // 16,)), dma((rows // 16,)),
        ],
        compiler_params=pltpu.CompilerParams(vmem_limit_bytes=16 * 1024 * 1024),
    )(own, fit, x)
    return mult.reshape(traces.shape), prim.reshape(traces.shape)


def solution(mesh):
    placed = P(None, "freq", "shot", None)
    return jax.shard_map(
        per_device,
        mesh=mesh,
        in_specs=(placed,),
        out_specs=(placed, placed),
        check_vma=False,
    )
```

```python
import functools
import math

import jax
import jax.numpy as jnp
from jax import lax
from jax.experimental import pallas as pl
from jax.experimental.pallas import tpu as pltpu
from jax.sharding import PartitionSpec as P

epsilon = 1e-06
SIDE = 4
MESH = pl.DeviceIdType.MESH
STEPS = (0, 1, -1, 2)


def kernel(
    dims, x_ref, own, fit_ref, a, b, prod, fit, plane,
    load_sem, own_sem, a_send, a_recv, b_send, b_recv, d_send, d_recv, o_send, o_recv, f_send, f_recv,
):
    freqs, rows, order, widths, plan = dims
    pieces = [piece for part in plan for piece in part]
    chunks = len(widths)
    starts = [sum(widths[:j]) for j in range(chunks)]
    block = order // SIDE
    scale = 1.0 / math.sqrt(order)
    f = lax.axis_index("freq")
    s = lax.axis_index("shot")
    c = lax.rem(s, 2)
    z = lax.rem(s // 2, SIDE)
    y = s // (2 * SIDE)
    p = z * (1 - c) + y * c
    q = y * (1 - c) + z * c

    def dev(qq, pp):
        return (1 - c) * ((qq * SIDE + pp) * 2) + c * ((pp * SIDE + qq) * 2 + 1)

    def turn(i, d):
        return lax.rem(i + d + SIDE, SIDE)

    ps = [turn(p, d) for d in STEPS]
    qs = [turn(q, d) for d in STEPS]
    pdev = [{"shot": dev(q, pp)} for pp in ps]
    qdev = [{"shot": dev(qq, p)} for qq in qs]
    sib = {"shot": s + 1 - 2 * c}

    ends = starts[1:] + [block]

    def lanes(i, j=None):
        j = i if j is None else j
        return pl.ds(starts[i], ends[j] - starts[i])

    def cols(qq, pp, i, j=None):
        j = i if j is None else j
        at = lax.rem(qq + pp, SIDE) * block + starts[i]
        return pl.ds(pl.multiple_of(at, 128), ends[j] - starts[i])

    def remote(src, dst, ss, rs, to):
        return pltpu.make_async_remote_copy(
            src_ref=src, dst_ref=dst, send_sem=ss, recv_sem=rs, device_id=to, device_id_type=MESH
        )

    def await_in(like, sem):
        remote(like, like, o_send, sem, sib).wait_recv()

    def await_out(like, sem):
        remote(like, like, sem, o_recv.at[0], sib).wait_send()

    load = pltpu.make_async_copy(x_ref, a.at[:, p], load_sem)
    load.start()

    barrier = pltpu.get_barrier_semaphore()
    ids = [(i, k) for i in range(freqs) for k in (0, 1) if i or k]
    fdev = [{"freq": lax.rem(f + i, freqs), "shot": s + k * (1 - 2 * c)} for i, k in ids]
    near = pdev[1:] + qdev[1:] + fdev
    for to in near:
        pl.semaphore_signal(barrier, inc=1, device_id=to, device_id_type=MESH)
    pl.semaphore_wait(barrier, len(near))
    load.wait()

    def send_a(n):
        h = (0, 1, 1, 0, 0, 1)[n]
        here = a.at[h, ps[(0, 0, 0, 0, 2, 1)[n]]]
        remote(here, here, a_send, a_recv.at[n], pdev[(1, 1, 2, 2, 1, 2)[n]]).start()

    def wait_a(n):
        await_in(a.at[(0, 1, 1, 0, 0, 1)[n], ps[(2, 2, 1, 1, 3, 3)[n]]], a_recv.at[n])

    def send_b(piece):
        n = pieces.index(piece)
        r, lo, hi = piece
        here = b.at[:, q * (1 - c) + ps[r] * c, ps[r] * (1 - c) + q * c, c, :, lanes(lo, hi)]
        for k in (1, 2, 3):
            remote(a.at[:, ps[r], :, cols(qs[k], p, lo, hi)], here, b_send, b_recv.at[n], qdev[k]).start()
        pltpu.make_async_copy(a.at[:, ps[r], :, cols(q, p, lo, hi)], here, own_sem.at[n]).start()

    def pass_b(piece):
        n = pieces.index(piece)
        r, lo, hi = piece
        mine = b.at[:, 0, 0, 0, :, lanes(lo, hi)]
        pltpu.make_async_copy(mine, mine, own_sem.at[n]).wait()
        await_in(b.at[:, 0, pl.ds(0, 3), 0, :, lanes(lo, hi)], b_recv.at[n])

        @pl.when(c == 0)
        def _():
            here = b.at[:, :, ps[r], 0, :, lanes(lo, hi)]
            remote(here, here, d_send, d_recv.at[n], sib).start()

        @pl.when(c == 1)
        def _():
            here = b.at[:, ps[r], :, 1, :, lanes(lo, hi)]
            remote(here, here, d_send, d_recv.at[n], sib).start()

    def wait_d(piece):
        await_in(b.at[:, 0, :, 0, :, lanes(*piece[1:])], d_recv.at[pieces.index(piece)])

    for n in (0, 2, 1, 3):
        send_a(n)
    for piece in plan[0]:
        send_b(piece)
    for n in (0, 2):
        wait_a(n)
        send_a(n // 2 + 4)
    for n in (1, 3):
        wait_a(n)
    for piece in plan[1]:
        send_b(piece)
    for n in (4, 5):
        wait_a(n)
    for piece in plan[2]:
        send_b(piece)

    def send_o(j):
        for k in (3, 1, 2):
            remote(
                prod.at[:, ps[k], :, lanes(j)], own.at[:, :, cols(q, p, j)], o_send, o_recv.at[j], pdev[k]
            ).start()

    sums = [jnp.zeros((8, 128), jnp.float32) for _ in range(3)]
    depth = SIDE * SIDE * 2 * rows
    passed = 0
    for j in range(chunks):
        width = widths[j]
        last = max(n for n, (r, lo, hi) in enumerate(pieces) if lo <= j)
        for piece in pieces[passed : last + 1]:
            pass_b(piece)
        for piece in pieces[passed : last + 1]:
            wait_d(piece)
        passed = max(passed, last + 1)
        here = cols(q, p, j)
        br = b[0, :, :, :, :, lanes(j)].reshape(depth, width)
        bi = b[1, :, :, :, :, lanes(j)].reshape(depth, width)
        for half in range(2):
            at = pl.ds(half * 2, 2)
            lhs = a[:, at].reshape(4 * rows, depth)
            if width == 128:
                x = jnp.dot(lhs, jnp.concatenate([br, bi], axis=1), preferred_element_type=jnp.float32)
                xr, xi = x[:, :128], x[:, 128:]
            else:
                xr = jnp.dot(lhs, br, preferred_element_type=jnp.float32)
                xi = jnp.dot(lhs, bi, preferred_element_type=jnp.float32)
            mr = (xr[: 2 * rows] - xi[2 * rows :]) * scale
            mi = (xi[: 2 * rows] + xr[2 * rows :]) * scale
            prod[0, at, :, lanes(j)] = mr.reshape(2, rows, width)
            prod[1, at, :, lanes(j)] = mi.reshape(2, rows, width)
            dr = a[0, at, :, here].reshape(2 * rows, width).astype(jnp.float32)
            di = a[1, at, :, here].reshape(2 * rows, width).astype(jnp.float32)
            terms = (mr * dr + mi * di, mr * di - mi * dr, mr * mr + mi * mi)
            for n, t in enumerate(terms):
                t = jnp.sum(t.reshape(-1, 8, width), axis=0)
                for w in range(0, width, 128):
                    sums[n] = sums[n] + t[:, w : w + 128]
        if j < chunks - 1:
            send_o(j)

    line = [jnp.sum(u, axis=0, keepdims=True) for u in sums]
    mine = fit.at[f * 2 + c]
    mine[...] = jnp.concatenate(line + [jnp.zeros((5, 128), jnp.float32)], axis=0)
    for to in fdev:
        remote(mine, mine, f_send.at[0], f_recv.at[0], to).start()
    send_o(chunks - 1)
    for j in range(chunks):
        own[:, :, cols(q, p, j)] = prod[:, p, :, lanes(j)]
    await_in(fit.at[pl.ds(0, len(fdev))], f_recv.at[0])
    here = plane.at[q * SIDE + p]
    here[...] = jnp.sum(fit[...], axis=0)
    others = [(i, k) for i in range(SIDE) for k in range(SIDE) if i or k]
    for i, k in others:
        remote(here, here, f_send.at[1], f_recv.at[1], {"shot": dev(qs[i], ps[k])}).start()
    await_in(plane.at[pl.ds(0, len(others))], f_recv.at[1])
    for j in range(chunks):
        await_in(prod.at[:, pl.ds(0, 3), :, lanes(j)], o_recv.at[j])
    fit_ref[...] = jnp.sum(plane[...], axis=0)
    await_out(a.at[:, pl.ds(0, 3)], a_send)
    await_out(b.at[:, pl.ds(0, 3), :, 0], b_send)
    await_out(b.at[:, :, :, 0], d_send)
    await_out(prod.at[:, pl.ds(0, 3)], o_send)
    await_out(fit.at[pl.ds(0, len(fdev))], f_send.at[0])
    await_out(plane.at[pl.ds(0, len(others))], f_send.at[1])


def finish(count, own, fit, x, mult_ref, prim_ref, mult, prim, m_sem, p_sem):
    total = jnp.sum(fit[...], axis=1, keepdims=True)
    den = total[2:3] / count + epsilon
    fit_re = total[0:1] / count / den
    fit_im = total[1:2] / count / den
    rows = own.shape[1]
    copies = []
    for n in range(rows // 16):
        at = pl.ds(n * 16, 16)
        mr, mi = own[0, at], own[1, at]
        mult[0, at] = mr.astype(jnp.bfloat16)
        mult[1, at] = mi.astype(jnp.bfloat16)
        copies.append(pltpu.make_async_copy(mult.at[:, at], mult_ref.at[:, at], m_sem.at[n]))
        copies[-1].start()
        dr, di = x[0, at].astype(jnp.float32), x[1, at].astype(jnp.float32)
        prim[0, at] = (dr - (fit_re * mr - fit_im * mi)).astype(jnp.bfloat16)
        prim[1, at] = (di - (fit_re * mi + fit_im * mr)).astype(jnp.bfloat16)
        copies.append(pltpu.make_async_copy(prim.at[:, at], prim_ref.at[:, at], p_sem.at[n]))
        copies[-1].start()
    for copy in copies:
        copy.wait()


def per_device(traces):
    rows, order = traces.shape[2], traces.shape[3]
    freqs = lax.axis_size("freq")
    block = order // SIDE
    widths = (256, 256, 256)
    chunks = len(widths)
    plan = ((), ((0, 0, 2), (2, 0, 1), (1, 0, 1)), ((3, 0, 0), (3, 1, 1), (2, 2, 2), (1, 2, 2), (3, 2, 2)))
    pieces = sum(len(part) for part in plan)
    dma = pltpu.SemaphoreType.DMA
    out = jax.ShapeDtypeStruct((2, rows, order), jnp.bfloat16)
    vmem = pl.BlockSpec(memory_space=pltpu.VMEM)
    x = traces.reshape(2, rows, order)
    anywhere = pl.BlockSpec(memory_space=pl.ANY)
    own, fit = pl.pallas_call(
        functools.partial(kernel, (freqs, rows, order, widths, plan)),
        out_shape=(
            jax.ShapeDtypeStruct((2, rows, order), jnp.float32),
            jax.ShapeDtypeStruct((8, 128), jnp.float32),
        ),
        in_specs=[pl.BlockSpec(memory_space=pltpu.HBM)],
        out_specs=(vmem, vmem),
        scratch_shapes=[
            pltpu.VMEM((2, SIDE, rows, order), jnp.bfloat16),
            pltpu.VMEM((2, SIDE, SIDE, 2, rows, block), jnp.bfloat16),
            pltpu.VMEM((2, SIDE, rows, block), jnp.float32),
            pltpu.VMEM((freqs * 2, 8, 128), jnp.float32),
            pltpu.VMEM((SIDE * SIDE, 8, 128), jnp.float32),
            dma, dma((pieces,)),
            dma, dma((6,)),
            dma, dma((pieces,)),
            dma, dma((pieces,)),
            dma, dma((chunks,)),
            dma((2,)), dma((2,)),
        ],
        compiler_params=pltpu.CompilerParams(
            collective_id=0, has_side_effects=True, vmem_limit_bytes=36 * 1024 * 1024
        ),
    )(pltpu.with_memory_space_constraint(x, pltpu.HBM))
    mult, prim = pl.pallas_call(
        functools.partial(finish, float(freqs * order * order)),
        out_shape=(out, out),
        in_specs=[vmem, vmem, vmem],
        out_specs=(anywhere, anywhere),
        scratch_shapes=[
            pltpu.VMEM((2, rows, order), jnp.bfloat16),
            pltpu.VMEM((2, rows, order), jnp.bfloat16),
            dma((rows // 16,)), dma((rows // 16,)),
        ],
        compiler_params=pltpu.CompilerParams(vmem_limit_bytes=16 * 1024 * 1024),
    )(own, fit, x)
    return mult.reshape(traces.shape), prim.reshape(traces.shape)


def solution(mesh):
    placed = P(None, "freq", "shot", None)
    return jax.shard_map(
        per_device,
        mesh=mesh,
        in_specs=(placed,),
        out_specs=(placed, placed),
        check_vma=False,
    )
```
